32 devices in a mesh: grp: 2 (over x), row: 16 (over z, y, core).
Axes of the slice: x: 2, y: 2, z: 4, core: 2. Of those that a mesh axis runs over, the one named last changes fastest.
Arguments:
- prior_basis: float32 [131072, 512], P(('grp', 'row')), parts along dimension 0, may hold values from -1 to 1, as said below
- samples: float32 [4, 131072, 64], P(None, ('grp', 'row')), parts along dimension 1, may hold values from -8 to 8
Outputs:
- new_basis: float32 [131072, 256], P(('grp', 'row')), parts along dimension 0
- leaf_estimates: float32 [4, 512], P(None, ('grp', 'row')), parts along dimension 1
The draws below stay inside these ranges and needn't reach their ends.
There are 2 independent parts, one for each index of `grp`. The reference program is written for one: setup_inputs(seed, part) draws one part's arguments, and reference() takes and returns one part's arrays. A program takes and returns all parts, laid end to end along the dimension named above; each array names one. Nothing has to cross between parts.
Inputs may be any that keep to these rules, and one draw needn't show every extreme that they name: The columns of prior_basis are orthonormal to float32 rounding.
All inputs are finite; a program needn't handle non-finite values.
Results may differ from the reference program's by a relative error of at most 0.0003.
Values sent between devices are 32-bit elements; how exact they have to be, the bound alone decides.
A program may use at most 64 MiB of HBM per device.

```python
import math
import jax
import jax.numpy as jnp
from jax import lax

ORDER = 65536
BASIS = 512
SAMPLES = 64
LEAF = 256
ROUNDS = 4
LEAVES = 256


def orthonormal_base(key):
    raw_block = jax.random.normal(jax.random.fold_in(key, 11), (ORDER, BASIS), jnp.float32)
    basis_q, upper = jnp.linalg.qr(raw_block)
    return basis_q


def draw_prior_basis(key, part):
    return orthonormal_base(key).astype(jnp.float32)


def draw_samples(key, part):
    basis_q = orthonormal_base(key)
    weights = jax.random.normal(jax.random.fold_in(key, 12), (ROUNDS, BASIS, SAMPLES), jnp.float32)
    weights = weights * jnp.sqrt(ORDER / BASIS)
    low_part = jnp.einsum('nk,rks->rns', basis_q, weights)
    leaf_scale = jnp.exp(jax.random.uniform(jax.random.fold_in(key, 13), (ROUNDS, LEAVES), jnp.float32, math.log(0.05), 0.0))
    row_scale = jnp.repeat(leaf_scale, LEAF, axis=1)[:, :, None]
    noise = jax.random.normal(jax.random.fold_in(key, 14), (ROUNDS, ORDER, SAMPLES), jnp.float32)
    return jnp.clip(low_part + row_scale * noise, -8.0, 8.0).astype(jnp.float32)


def setup_inputs(seed: int = 0, part: int = 0) -> dict:
    splits = jax.random.split(jax.random.key(seed), 3)
    own_keys = jax.random.split(jax.random.fold_in(splits[2], part), 3)
    return {
        "prior_basis": draw_prior_basis(jax.random.fold_in(jax.random.fold_in(splits[2], part), 71), part),
        "samples": draw_samples(jax.random.fold_in(jax.random.fold_in(splits[2], part), 71), part),
    }


def reference(prior_basis, samples):
    highest = lax.Precision.HIGHEST
    new_cols = []
    estimates = []
    for number in range(ROUNDS):
        sample_block = samples[number]
        energy = jnp.sum(sample_block * sample_block)
        c_prior = jnp.dot(prior_basis.T, sample_block, precision=highest)
        remainder = sample_block - jnp.dot(prior_basis, c_prior, precision=highest)
        if new_cols:
            added = jnp.concatenate(new_cols, axis=1)
            c_added = jnp.dot(added.T, sample_block, precision=highest)
            remainder = remainder - jnp.dot(added, c_added, precision=highest)
        gram = jnp.dot(remainder.T, remainder, precision=highest)
        factor = jnp.linalg.cholesky(gram)
        fresh_cols = jax.scipy.linalg.solve_triangular(factor, remainder.T, lower=True).T
        leaf_energy = lax.optimization_barrier(jnp.sum((remainder * remainder).reshape(LEAVES, LEAF, SAMPLES), axis=(1, 2)))
        estimates.append(jnp.sqrt(LEAVES * leaf_energy / energy))
        new_cols.append(fresh_cols)
    return (jnp.concatenate(new_cols, axis=1), jnp.stack(estimates))
```

```python
import functools

import jax
import jax.numpy as jnp
from jax import lax
from jax.experimental import pallas as pl
from jax.experimental.pallas import tpu as pltpu
from jax.sharding import PartitionSpec as P

LEAF = 256
TILE = 512
F32 = jnp.float32
BF16 = jnp.bfloat16
NN = (((1,), (0,)), ((), ()))
NT = (((1,), (1,)), ((), ()))
TN = (((0,), (0,)), ((), ()))


def split(x):
    hi = x.astype(BF16)
    return hi, (x - hi.astype(F32)).astype(BF16)


def dot(a, b, dims=NN):
    return lax.dot_general(a, b, dims, preferred_element_type=F32)


def exact(a, b, dims=NN):
    return lax.dot_general(
        a, b, dims, precision=lax.Precision.HIGHEST, preferred_element_type=F32
    )


def stats_kernel(p_ref, s_ref, o_ref):
    rounds = s_ref.shape[0]
    basis = p_ref.shape[1]

    @pl.when(pl.program_id(0) == 0)
    def _():
        o_ref[...] = jnp.zeros_like(o_ref)

    st = jnp.concatenate([s_ref[r].T for r in range(rounds)], axis=0)
    sh, sl = split(st)
    ph, plo = split(p_ref[...])
    o_ref[:, :basis] += dot(sh, ph) + dot(sl, ph) + dot(sh, plo)
    o_ref[:, basis:] += dot(sh, sh, NT) + dot(sl, sh, NT) + dot(sh, sl, NT)


def factor_block(block):
    size = block.shape[0]
    width = 2 * size
    groups = size // 8
    eye = (
        lax.broadcasted_iota(jnp.int32, (size, size), 0)
        == lax.broadcasted_iota(jnp.int32, (size, size), 1)
    ).astype(F32)
    aug = jnp.concatenate([block, eye], axis=1)
    rows = [aug[8 * g : 8 * g + 8, :] for g in range(groups)]
    sub = lax.broadcasted_iota(jnp.int32, (8, width), 0)
    for p in range(groups):
        cols = {
            g: [
                jnp.broadcast_to(rows[g][:, 8 * p + j : 8 * p + j + 1], (8, width))
                for j in range(8)
            ]
            for g in range(p, groups)
        }
        v = rows[p]
        scale = jnp.zeros((8, width), F32)
        scaled = []
        for k in range(8):
            d = cols[p][k][k : k + 1, :]
            rinv = 1.0 / d
            scale = jnp.where(sub == k, jnp.broadcast_to(lax.rsqrt(d), (8, width)), scale)
            vk = v[k : k + 1, :] * rinv
            scaled.append(vk)
            below = jnp.where(sub > k, cols[p][k], 0.0)
            steps = {j: cols[p][j][k : k + 1, :] * rinv for j in range(k + 1, 8)}
            for j in range(k + 1, 8):
                cols[p][j] = cols[p][j] - below * steps[j]
            v = v - below * vk
            for g in range(p + 1, groups):
                for j in range(k + 1, 8):
                    cols[g][j] = cols[g][j] - cols[g][k] * steps[j]
        for g in range(p + 1, groups):
            for k in range(8):
                rows[g] = rows[g] - cols[g][k] * scaled[k]
        rows[p] = v * scale
    return jnp.concatenate(rows, axis=0)


def factor_kernel(columns, x_ref, w_ref, lt_ref, e_ref, ae_ref):
    total = x_ref.shape[0]
    basis = x_ref.shape[1] - total
    rounds = total // columns
    ct = x_ref[:, :basis]
    g = x_ref[:, basis:]
    row = lax.broadcasted_iota(jnp.int32, (total, total), 0)
    col = lax.broadcasted_iota(jnp.int32, (total, total), 1)
    eye = row == col
    diag = jnp.sum(jnp.where(eye, g, 0.0), axis=1, keepdims=True)
    for r in range(rounds):
        e_ref[r : r + 1, :] = jnp.broadcast_to(
            jnp.sum(diag[r * columns : (r + 1) * columns, :], axis=0, keepdims=True),
            (1, e_ref.shape[1]),
        )
    ae_ref[:, :total] = g - exact(ct, ct, NT)
    ae_ref[:, total:] = eye.astype(F32)
    lt_ref[...] = jnp.zeros_like(lt_ref)
    for r in range(rounds):
        lo, hi = r * columns, (r + 1) * columns
        both = factor_block(ae_ref[lo:hi, lo:hi])
        upper = (
            lax.broadcasted_iota(jnp.int32, (columns, columns), 0)
            <= lax.broadcasted_iota(jnp.int32, (columns, columns), 1)
        )
        lt_ref[lo:hi, lo:hi] = jnp.where(upper, both[:, :columns], 0.0)
        z = exact(both[:, columns:], ae_ref[lo:hi, :])
        ae_ref[lo:hi, :] = z
        if r + 1 < rounds:
            ae_ref[hi:, :] -= exact(z[:, hi:total], z, TN)
    linv = ae_ref[:, total:]
    w_ref[:, :basis] = -exact(linv, ct)
    w_ref[:, basis:] = linv


def final_kernel(total_leaves, columns, p_ref, s_ref, w_ref, lt_ref, e_ref, n_ref, q_ref, wh, wl, lh, ll, sums):
    rounds = s_ref.shape[0]
    tile, basis = p_ref.shape
    step = pl.program_id(0)
    per = tile // LEAF

    @pl.when(step == 0)
    def _():
        h, l = split(w_ref[...])
        wh[...] = h
        wl[...] = l
        h, l = split(lt_ref[...])
        lh[...] = h
        ll[...] = l

    s = jnp.concatenate([s_ref[r] for r in range(rounds)], axis=1)
    sh, sl = split(s)
    ph, plo = split(p_ref[...])
    ah, al = wh[:, :basis], wl[:, :basis]
    bh, bl = wh[:, basis:], wl[:, basis:]
    out = (
        dot(ph, ah, NT) + dot(plo, ah, NT) + dot(ph, al, NT)
        + dot(sh, bh, NT) + dot(sl, bh, NT) + dot(sh, bl, NT)
    )
    n_ref[...] = out
    nh, nl = split(out)
    rem = dot(nh, lh[...]) + dot(nl, lh[...]) + dot(nh, ll[...])
    sq = rem * rem
    for i in range(per):
        sums[pl.ds(step * per + i, 1), :] = jnp.sum(
            sq[i * LEAF : (i + 1) * LEAF, :], axis=0, keepdims=True
        )

    @pl.when(step == pl.num_programs(0) - 1)
    def _():
        width = rounds * columns
        pick = (
            lax.broadcasted_iota(jnp.int32, (rounds, width), 1) // columns
            == lax.broadcasted_iota(jnp.int32, (rounds, width), 0)
        ).astype(F32)
        leaf = exact(pick, sums[...], NT)
        q_ref[...] = jnp.sqrt(total_leaves * leaf / e_ref[:rounds, :1])


def local(prior_basis, samples):
    rounds, rows, columns = samples.shape
    basis = prior_basis.shape[1]
    total = rounds * columns
    tile = min(TILE, rows)
    leaves = rows // LEAF
    total_leaves = leaves * lax.axis_size("row")
    grid = (rows // tile,)
    p_spec = pl.BlockSpec((tile, basis), lambda i: (i, 0))
    s_spec = pl.BlockSpec((rounds, tile, columns), lambda i: (0, i, 0))
    whole = lambda *shape: pl.BlockSpec(shape, lambda i: (0,) * len(shape))
    part = pl.pallas_call(
        stats_kernel,
        grid=grid,
        in_specs=[p_spec, s_spec],
        out_specs=whole(total, basis + total),
        out_shape=jax.ShapeDtypeStruct((total, basis + total), F32),
        name="stats",
    )(prior_basis, samples)
    stat = lax.psum(part, "row")
    w, lt, energy = pl.pallas_call(
        functools.partial(factor_kernel, columns),
        out_shape=(
            jax.ShapeDtypeStruct((total, basis + total), F32),
            jax.ShapeDtypeStruct((total, total), F32),
            jax.ShapeDtypeStruct((8, 128), F32),
        ),
        scratch_shapes=[pltpu.VMEM((total, 2 * total), F32)],
        name="factor",
    )(stat)
    return pl.pallas_call(
        functools.partial(final_kernel, total_leaves, columns),
        grid=grid,
        in_specs=[p_spec, s_spec, whole(total, basis + total), whole(total, total), whole(8, 128)],
        out_specs=(pl.BlockSpec((tile, total), lambda i: (i, 0)), whole(rounds, leaves)),
        out_shape=(
            jax.ShapeDtypeStruct((rows, total), F32),
            jax.ShapeDtypeStruct((rounds, leaves), F32),
        ),
        scratch_shapes=[
            pltpu.VMEM((total, basis + total), BF16),
            pltpu.VMEM((total, basis + total), BF16),
            pltpu.VMEM((total, total), BF16),
            pltpu.VMEM((total, total), BF16),
            pltpu.VMEM((leaves, total), F32),
        ],
        name="final",
    )(prior_basis, samples, w, lt, energy)


def solution(mesh):
    in_specs = (P(("grp", "row"), None), P(None, ("grp", "row"), None))
    out_specs = (P(("grp", "row"), None), P(None, ("grp", "row")))
    return jax.shard_map(local, mesh=mesh, in_specs=in_specs, out_specs=out_specs, check_vma=False)
```

```python
import functools

import jax
import jax.numpy as jnp
from jax import lax
from jax.experimental import pallas as pl
from jax.experimental.pallas import tpu as pltpu
from jax.sharding import PartitionSpec as P

LEAF = 256
TILE = 512
F32 = jnp.float32
BF16 = jnp.bfloat16
MESH = pl.DeviceIdType.MESH
NN = (((1,), (0,)), ((), ()))
NT = (((1,), (1,)), ((), ()))
TN = (((0,), (0,)), ((), ()))


def split(x):
    hi = x.astype(BF16)
    return hi, (x - hi.astype(F32)).astype(BF16)


def dot(a, b, dims=NN):
    return lax.dot_general(a, b, dims, preferred_element_type=F32)


def exact(a, b, dims=NN):
    return lax.dot_general(
        a, b, dims, precision=lax.Precision.HIGHEST, preferred_element_type=F32
    )


def stats_kernel(p_ref, s_ref, o_ref):
    rounds = s_ref.shape[0]
    basis = p_ref.shape[1]

    @pl.when(pl.program_id(0) == 0)
    def _():
        o_ref[...] = jnp.zeros_like(o_ref)

    st = jnp.concatenate([s_ref[r] for r in range(rounds)], axis=0)
    sh, sl = split(st)
    ph, plo = split(p_ref[...])
    o_ref[:, :basis] += dot(sh, ph) + dot(sl, ph) + dot(sh, plo)
    o_ref[:, basis:] += dot(sh, sh, NT) + dot(sl, sh, NT) + dot(sh, sl, NT)


def sum_kernel(m, x_ref, o_ref, pair, part, got, total, pair_send, pair_recv, rs_send, rs_recv, ag_send, ag_recv, fw_send, fw_recv):
    me = lax.axis_index("row")
    core = lax.rem(me, 2)
    chip = me // 2
    mate = me + 1 - 2 * core
    offsets = sorted(range(1, m), key=lambda i: abs(i - m // 2))
    peers = [lax.rem(chip + i, m) for i in offsets]

    barrier = pltpu.get_barrier_semaphore()
    for device in [mate] + [2 * t + core for t in peers]:
        pl.semaphore_signal(barrier, inc=1, device_id={"row": device}, device_id_type=MESH)
    pl.semaphore_wait(barrier, m)

    def copy(src, dst, send, recv, device):
        return pltpu.make_async_remote_copy(
            src_ref=src, dst_ref=dst, send_sem=send, recv_sem=recv,
            device_id={"row": device}, device_id_type=MESH,
        )

    order = peers + [chip]
    first = [
        copy(x_ref.at[2 * t + 1 - core], pair.at[t], pair_send.at[t], pair_recv.at[t], mate)
        for t in order
    ]
    for c in first:
        c.start()
    second = []
    for i, t in enumerate(order):
        first[i].wait_recv()
        part[t] = x_ref[2 * t + core] + pair[t]
        if t is not chip:
            c = copy(part.at[t], got.at[chip], rs_send.at[t], rs_recv.at[chip], 2 * t + core)
            c.start()
            second.append(c)

    def arrived(src, dst, recv):
        return pltpu.make_async_copy(src, dst, recv)

    value = part[chip]
    for t in reversed(peers):
        arrived(got.at[t], got.at[t], rs_recv.at[t]).wait()
        value = value + got[t]
    total[...] = value
    o_ref[me] = value
    third = [copy(total, o_ref.at[me], ag_send.at[t], ag_recv.at[chip], 2 * t + core) for t in peers]
    for c in third:
        c.start()
    last = [copy(total, o_ref.at[me], fw_send.at[chip], fw_recv.at[chip], mate)]
    last[0].start()
    for t in reversed(peers):
        block = o_ref.at[2 * t + core]
        arrived(block, block, ag_recv.at[t]).wait()
        c = copy(block, block, fw_send.at[t], fw_recv.at[t], mate)
        c.start()
        last.append(c)
    for t in order:
        block = o_ref.at[2 * t + 1 - core]
        arrived(block, block, fw_recv.at[t]).wait()
    for c in first + second + third + last:
        c.wait_send()


def all_sum(x):
    n = lax.axis_size("row")
    m = n // 2
    rows, width = x.shape
    chunk = (rows // n, width)
    vmem = pl.BlockSpec(memory_space=pltpu.VMEM)
    out = pl.pallas_call(
        functools.partial(sum_kernel, m),
        in_specs=[vmem],
        out_specs=vmem,
        out_shape=jax.ShapeDtypeStruct((n,) + chunk, F32),
        scratch_shapes=[
            pltpu.VMEM((m,) + chunk, F32),
            pltpu.VMEM((m,) + chunk, F32),
            pltpu.VMEM((m,) + chunk, F32),
            pltpu.VMEM(chunk, F32),
        ]
        + [pltpu.SemaphoreType.DMA((m,))] * 8,
        compiler_params=pltpu.CompilerParams(collective_id=0, has_side_effects=True),
        name="all_sum",
    )(x.reshape((n,) + chunk))
    return out.reshape(rows, width)


def factor_block(block):
    size = block.shape[0]
    width = 2 * size
    groups = size // 8
    eye = (
        lax.broadcasted_iota(jnp.int32, (size, size), 0)
        == lax.broadcasted_iota(jnp.int32, (size, size), 1)
    ).astype(F32)
    aug = jnp.concatenate([block, eye], axis=1)
    rows = [aug[8 * g : 8 * g + 8, :] for g in range(groups)]
    sub = lax.broadcasted_iota(jnp.int32, (8, width), 0)
    for p in range(groups):
        cols = {
            g: [
                jnp.broadcast_to(rows[g][:, 8 * p + j : 8 * p + j + 1], (8, width))
                for j in range(8)
            ]
            for g in range(p, groups)
        }
        v = rows[p]
        scale = jnp.zeros((8, width), F32)
        scaled = []
        for k in range(8):
            d = cols[p][k][k : k + 1, :]
            rinv = 1.0 / d
            scale = jnp.where(sub == k, jnp.broadcast_to(lax.rsqrt(d), (8, width)), scale)
            vk = v[k : k + 1, :] * rinv
            scaled.append(vk)
            below = jnp.where(sub > k, cols[p][k], 0.0)
            steps = {j: cols[p][j][k : k + 1, :] * rinv for j in range(k + 1, 8)}
            for j in range(k + 1, 8):
                cols[p][j] = cols[p][j] - below * steps[j]
            v = v - below * vk
            for g in range(p + 1, groups):
                for j in range(k + 1, 8):
                    cols[g][j] = cols[g][j] - cols[g][k] * steps[j]
        for g in range(p + 1, groups):
            for k in range(8):
                rows[g] = rows[g] - cols[g][k] * scaled[k]
        rows[p] = v * scale
    return jnp.concatenate(rows, axis=0)


def factor_kernel(columns, x_ref, w_ref, lt_ref, e_ref, ae_ref):
    total = x_ref.shape[0]
    basis = x_ref.shape[1] - total
    rounds = total // columns
    ct = x_ref[:, :basis]
    g = x_ref[:, basis:]
    row = lax.broadcasted_iota(jnp.int32, (total, total), 0)
    col = lax.broadcasted_iota(jnp.int32, (total, total), 1)
    eye = row == col
    diag = jnp.sum(jnp.where(eye, g, 0.0), axis=1, keepdims=True)
    for r in range(rounds):
        e_ref[r : r + 1, :] = jnp.broadcast_to(
            jnp.sum(diag[r * columns : (r + 1) * columns, :], axis=0, keepdims=True),
            (1, e_ref.shape[1]),
        )
    ae_ref[:, :total] = g - exact(ct, ct, NT)
    ae_ref[:, total:] = eye.astype(F32)
    lt_ref[...] = jnp.zeros_like(lt_ref)
    for r in range(rounds):
        lo, hi = r * columns, (r + 1) * columns
        both = factor_block(ae_ref[lo:hi, lo:hi])
        upper = (
            lax.broadcasted_iota(jnp.int32, (columns, columns), 0)
            <= lax.broadcasted_iota(jnp.int32, (columns, columns), 1)
        )
        lt_ref[lo:hi, lo:hi] = jnp.where(upper, both[:, :columns], 0.0)
        z = exact(both[:, columns:], ae_ref[lo:hi, :])
        ae_ref[lo:hi, :] = z
        if r + 1 < rounds:
            ae_ref[hi:, :] -= exact(z[:, hi:total], z, TN)
    linv = ae_ref[:, total:]
    w_ref[:, :basis] = -exact(linv, ct)
    w_ref[:, basis:] = linv


def final_kernel(total_leaves, columns, p_ref, s_ref, w_ref, lt_ref, e_ref, n_ref, q_ref, wh, wl, lh, ll, sums):
    rounds = s_ref.shape[0]
    tile, basis = p_ref.shape
    step = pl.program_id(0)
    per = tile // LEAF

    @pl.when(step == 0)
    def _():
        h, l = split(w_ref[...])
        wh[...] = h
        wl[...] = l
        h, l = split(lt_ref[...])
        lh[...] = h
        ll[...] = l

    s = jnp.concatenate([s_ref[r] for r in range(rounds)], axis=0).T
    sh, sl = split(s)
    ph, plo = split(p_ref[...])
    ah, al = wh[:, :basis], wl[:, :basis]
    bh, bl = wh[:, basis:], wl[:, basis:]
    out = (
        dot(ph, ah, NT) + dot(plo, ah, NT) + dot(ph, al, NT)
        + dot(sh, bh, NT) + dot(sl, bh, NT) + dot(sh, bl, NT)
    )
    n_ref[...] = out
    nh, nl = split(out)
    rem = dot(nh, lh[...]) + dot(nl, lh[...]) + dot(nh, ll[...])
    sq = rem * rem
    for i in range(per):
        sums[pl.ds(step * per + i, 1), :] = jnp.sum(
            sq[i * LEAF : (i + 1) * LEAF, :], axis=0, keepdims=True
        )

    @pl.when(step == pl.num_programs(0) - 1)
    def _():
        width = rounds * columns
        pick = (
            lax.broadcasted_iota(jnp.int32, (rounds, width), 1) // columns
            == lax.broadcasted_iota(jnp.int32, (rounds, width), 0)
        ).astype(F32)
        leaf = exact(pick, sums[...], NT)
        q_ref[...] = jnp.sqrt(total_leaves * leaf / e_ref[:rounds, :1])


def local(prior_basis, samples):
    rounds, rows, columns = samples.shape
    basis = prior_basis.shape[1]
    total = rounds * columns
    tile = min(TILE, rows)
    leaves = rows // LEAF
    total_leaves = leaves * lax.axis_size("row")
    grid = (rows // tile,)
    p_spec = pl.BlockSpec((tile, basis), lambda i: (i, 0))
    samples = jnp.swapaxes(samples, 1, 2)
    s_spec = pl.BlockSpec((rounds, columns, tile), lambda i: (0, 0, i))
    whole = lambda *shape: pl.BlockSpec(shape, lambda i: (0,) * len(shape))
    part = pl.pallas_call(
        stats_kernel,
        grid=grid,
        in_specs=[p_spec, s_spec],
        out_specs=whole(total, basis + total),
        out_shape=jax.ShapeDtypeStruct((total, basis + total), F32),
        name="stats",
    )(prior_basis, samples)
    stat = all_sum(part)
    w, lt, energy = pl.pallas_call(
        functools.partial(factor_kernel, columns),
        out_shape=(
            jax.ShapeDtypeStruct((total, basis + total), F32),
            jax.ShapeDtypeStruct((total, total), F32),
            jax.ShapeDtypeStruct((8, 128), F32),
        ),
        scratch_shapes=[pltpu.VMEM((total, 2 * total), F32)],
        name="factor",
    )(stat)
    return pl.pallas_call(
        functools.partial(final_kernel, total_leaves, columns),
        grid=grid,
        in_specs=[p_spec, s_spec, whole(total, basis + total), whole(total, total), whole(8, 128)],
        out_specs=(pl.BlockSpec((tile, total), lambda i: (i, 0)), whole(rounds, leaves)),
        out_shape=(
            jax.ShapeDtypeStruct((rows, total), F32),
            jax.ShapeDtypeStruct((rounds, leaves), F32),
        ),
        scratch_shapes=[
            pltpu.VMEM((total, basis + total), BF16),
            pltpu.VMEM((total, basis + total), BF16),
            pltpu.VMEM((total, total), BF16),
            pltpu.VMEM((total, total), BF16),
            pltpu.VMEM((leaves, total), F32),
        ],
        name="final",
    )(prior_basis, samples, w, lt, energy)


def solution(mesh):
    in_specs = (P(("grp", "row"), None), P(None, ("grp", "row"), None))
    out_specs = (P(("grp", "row"), None), P(None, ("grp", "row")))
    return jax.shard_map(local, mesh=mesh, in_specs=in_specs, out_specs=out_specs, check_vma=False)
```

```python
import functools

import jax
import jax.numpy as jnp
from jax import lax
from jax.experimental import pallas as pl
from jax.experimental.pallas import tpu as pltpu
from jax.sharding import PartitionSpec as P

LEAF = 256
LANES = 128
TILE = 512
F32 = jnp.float32
BF16 = jnp.bfloat16
MESH = pl.DeviceIdType.MESH
NN = (((1,), (0,)), ((), ()))
NT = (((1,), (1,)), ((), ()))
TN = (((0,), (0,)), ((), ()))


def split(x):
    hi = x.astype(BF16)
    return hi, (x - hi.astype(F32)).astype(BF16)


def dot(a, b, dims=NN):
    return lax.dot_general(a, b, dims, preferred_element_type=F32)


def exact(a, b, dims=NN):
    return lax.dot_general(
        a, b, dims, precision=lax.Precision.HIGHEST, preferred_element_type=F32
    )


def blocks(total, basis):
    n, b = total // LANES, basis // LANES
    return [(i, j) for i in range(n) for j in range(b)] + [
        (i, b + j) for i in range(n) for j in range(i + 1)
    ]


def unpack(x_ref, total, basis):
    place = {k: i for i, k in enumerate(blocks(total, basis))}
    n, b = total // LANES, basis // LANES

    def block(i, j):
        if j >= b and j - b > i:
            return block(j - b, b + i).T
        k = place[i, j]
        return x_ref[k * LANES : (k + 1) * LANES, :]

    full = [[block(i, j) for j in range(b + n)] for i in range(n)]
    rows = [jnp.concatenate(line, axis=1) for line in full]
    out = jnp.concatenate(rows, axis=0)
    return out[:, :basis], out[:, basis:]


def stats_kernel(p_ref, s_ref, o_ref):
    rounds, columns = s_ref.shape[:2]
    basis = p_ref.shape[1]

    @pl.when(pl.program_id(0) == 0)
    def _():
        o_ref[...] = jnp.zeros_like(o_ref)

    st = jnp.concatenate([s_ref[r] for r in range(rounds)], axis=0)
    sh, sl = split(st)
    ph, plo = split(p_ref[...])
    c = dot(sh, ph) + dot(sl, ph) + dot(sh, plo)
    g = dot(sh, sh, NT) + dot(sl, sh, NT) + dot(sh, sl, NT)
    x = jnp.concatenate([c, g], axis=1)
    for k, (i, j) in enumerate(blocks(rounds * columns, basis)):
        o_ref[k * LANES : (k + 1) * LANES, :] += x[
            i * LANES : (i + 1) * LANES, j * LANES : (j + 1) * LANES
        ]


def sum_kernel(line, x_ref, o_ref, pair, mine, theirs, beside, ready, got, total, pair_send, pair_recv, y_send, y_recv, z_send, z_recv, oz_send, oz_recv, oy_send, oy_recv, oc_send, oc_recv):
    me = lax.axis_index("row")
    core = lax.rem(me, 2)
    y = lax.rem(me // 2, 2)
    z = me // 4
    mate = me + 1 - 2 * core
    next_y = me + 2 - 4 * y
    offsets = sorted(range(1, line), key=lambda i: abs(i - line // 2))
    peers = [lax.rem(z + i, line) for i in offsets]
    order = peers + [z]

    def device(t):
        return 4 * t + 2 * y + core

    barrier = pltpu.get_barrier_semaphore()
    for other in [mate, next_y] + [device(t) for t in peers]:
        pl.semaphore_signal(barrier, inc=1, device_id={"row": other}, device_id_type=MESH)
    pl.semaphore_wait(barrier, line + 1)

    started = []

    def send(src, dst, send_sem, recv_sem, other):
        c = pltpu.make_async_remote_copy(
            src_ref=src, dst_ref=dst, send_sem=send_sem, recv_sem=recv_sem,
            device_id={"row": other}, device_id_type=MESH,
        )
        c.start()
        started.append(c)

    def arrived(block, recv_sem):
        pltpu.make_async_copy(block, block, recv_sem).wait()

    for t in order:
        send(x_ref.at[1 - core, :, t], pair.at[:, t], pair_send.at[t], pair_recv.at[t], mate)
    for t in order:
        arrived(pair.at[:, t], pair_recv.at[t])
        theirs[t] = x_ref[core, 1 - y, t] + pair[1 - y, t]
        mine[t] = x_ref[core, y, t] + pair[y, t]
        send(theirs.at[t], beside.at[t], y_send.at[t], y_recv.at[t], next_y)
    for t in peers:
        arrived(beside.at[t], y_recv.at[t])
        ready[t] = mine[t] + beside[t]
        send(ready.at[t], got.at[z], z_send.at[t], z_recv.at[z], device(t))
    arrived(beside.at[z], y_recv.at[z])
    value = mine[z] + beside[z]
    for t in reversed(peers):
        arrived(got.at[t], z_recv.at[t])
        value = value + got[t]
    total[...] = value
    home = o_ref.at[core, y, z]
    o_ref[core, y, z] = value
    for t in peers:
        send(total, home, oz_send.at[t], oz_recv.at[z], device(t))
    send(total, home, oy_send.at[z], oy_recv.at[z], next_y)
    send(total, home, oc_send.at[y, z], oc_recv.at[y, z], mate)
    back = [z] + list(reversed(peers))
    for i, t in enumerate(back):
        if i:
            block = o_ref.at[core, y, t]
            arrived(block, oz_recv.at[t])
            send(block, block, oy_send.at[t], oy_recv.at[t], next_y)
            send(block, block, oc_send.at[y, t], oc_recv.at[y, t], mate)
    for t in back:
        block = o_ref.at[core, 1 - y, t]
        arrived(block, oy_recv.at[t])
        send(block, block, oc_send.at[1 - y, t], oc_recv.at[1 - y, t], mate)
    for t in back:
        for side in range(2):
            arrived(o_ref.at[1 - core, side, t], oc_recv.at[side, t])
    for c in started:
        c.wait_send()


def all_sum(x):
    n = lax.axis_size("row")
    line = n // 4
    rows, width = x.shape
    chunk = (rows // n, width)
    vmem = pl.BlockSpec(memory_space=pltpu.VMEM)
    sem = pltpu.SemaphoreType.DMA
    out = pl.pallas_call(
        functools.partial(sum_kernel, line),
        in_specs=[vmem],
        out_specs=vmem,
        out_shape=jax.ShapeDtypeStruct((2, 2, line) + chunk, F32),
        scratch_shapes=[pltpu.VMEM((2, line) + chunk, F32)]
        + [pltpu.VMEM((line,) + chunk, F32)] * 5
        + [pltpu.VMEM(chunk, F32)]
        + [sem((line,))] * 10
        + [sem((2, line))] * 2,
        compiler_params=pltpu.CompilerParams(collective_id=0, has_side_effects=True),
        name="all_sum",
    )(x.reshape((2, 2, line) + chunk))
    return out.reshape(rows, width)


def factor_block(block):
    size = block.shape[0]
    width = 2 * size
    groups = size // 8
    eye = (
        lax.broadcasted_iota(jnp.int32, (size, size), 0)
        == lax.broadcasted_iota(jnp.int32, (size, size), 1)
    ).astype(F32)
    aug = jnp.concatenate([block, eye], axis=1)
    rows = [aug[8 * g : 8 * g + 8, :] for g in range(groups)]
    sub = lax.broadcasted_iota(jnp.int32, (8, width), 0)
    for p in range(groups):
        cols = {
            g: [
                jnp.broadcast_to(rows[g][:, 8 * p + j : 8 * p + j + 1], (8, width))
                for j in range(8)
            ]
            for g in range(p, groups)
        }
        v = rows[p]
        scale = jnp.zeros((8, width), F32)
        scaled = []
        for k in range(8):
            d = cols[p][k][k : k + 1, :]
            rinv = 1.0 / d
            scale = jnp.where(sub == k, jnp.broadcast_to(lax.rsqrt(d), (8, width)), scale)
            vk = v[k : k + 1, :] * rinv
            scaled.append(vk)
            below = jnp.where(sub > k, cols[p][k], 0.0)
            steps = {j: cols[p][j][k : k + 1, :] * rinv for j in range(k + 1, 8)}
            for j in range(k + 1, 8):
                cols[p][j] = cols[p][j] - below * steps[j]
            v = v - below * vk
            for g in range(p + 1, groups):
                for j in range(k + 1, 8):
                    cols[g][j] = cols[g][j] - cols[g][k] * steps[j]
        for g in range(p + 1, groups):
            for k in range(8):
                rows[g] = rows[g] - cols[g][k] * scaled[k]
        rows[p] = v * scale
    return jnp.concatenate(rows, axis=0)


def factor_kernel(columns, x_ref, w_ref, lt_ref, e_ref, ae_ref):
    total = lt_ref.shape[0]
    basis = w_ref.shape[1] - total
    rounds = total // columns
    ct, g = unpack(x_ref, total, basis)
    row = lax.broadcasted_iota(jnp.int32, (total, total), 0)
    col = lax.broadcasted_iota(jnp.int32, (total, total), 1)
    eye = row == col
    diag = jnp.sum(jnp.where(eye, g, 0.0), axis=1, keepdims=True)
    for r in range(rounds):
        e_ref[r : r + 1, :] = jnp.broadcast_to(
            jnp.sum(diag[r * columns : (r + 1) * columns, :], axis=0, keepdims=True),
            (1, e_ref.shape[1]),
        )
    ae_ref[:, :total] = g - exact(ct, ct, NT)
    ae_ref[:, total:] = eye.astype(F32)
    lt_ref[...] = jnp.zeros_like(lt_ref)
    for r in range(rounds):
        lo, hi = r * columns, (r + 1) * columns
        both = factor_block(ae_ref[lo:hi, lo:hi])
        upper = (
            lax.broadcasted_iota(jnp.int32, (columns, columns), 0)
            <= lax.broadcasted_iota(jnp.int32, (columns, columns), 1)
        )
        lt_ref[lo:hi, lo:hi] = jnp.where(upper, both[:, :columns], 0.0)
        z = exact(both[:, columns:], ae_ref[lo:hi, :])
        ae_ref[lo:hi, :] = z
        if r + 1 < rounds:
            ae_ref[hi:, :] -= exact(z[:, hi:total], z, TN)
    linv = ae_ref[:, total:]
    w_ref[:, :basis] = -exact(linv, ct)
    w_ref[:, basis:] = linv


def final_kernel(total_leaves, columns, p_ref, s_ref, w_ref, lt_ref, e_ref, n_ref, q_ref, wh, wl, lh, ll, sums):
    rounds = s_ref.shape[0]
    tile, basis = p_ref.shape
    step = pl.program_id(0)
    per = tile // LEAF

    @pl.when(step == 0)
    def _():
        h, l = split(w_ref[...])
        wh[...] = h
        wl[...] = l
        h, l = split(lt_ref[...])
        lh[...] = h
        ll[...] = l

    s = jnp.concatenate([s_ref[r] for r in range(rounds)], axis=0).T
    sh, sl = split(s)
    ph, plo = split(p_ref[...])
    ah, al = wh[:, :basis], wl[:, :basis]
    bh, bl = wh[:, basis:], wl[:, basis:]
    out = (
        dot(ph, ah, NT) + dot(plo, ah, NT) + dot(ph, al, NT)
        + dot(sh, bh, NT) + dot(sl, bh, NT) + dot(sh, bl, NT)
    )
    n_ref[...] = out
    nh, nl = split(out)
    rem = dot(nh, lh[...]) + dot(nl, lh[...]) + dot(nh, ll[...])
    sq = rem * rem
    for i in range(per):
        sums[pl.ds(step * per + i, 1), :] = jnp.sum(
            sq[i * LEAF : (i + 1) * LEAF, :], axis=0, keepdims=True
        )

    @pl.when(step == pl.num_programs(0) - 1)
    def _():
        width = rounds * columns
        pick = (
            lax.broadcasted_iota(jnp.int32, (rounds, width), 1) // columns
            == lax.broadcasted_iota(jnp.int32, (rounds, width), 0)
        ).astype(F32)
        leaf = exact(pick, sums[...], NT)
        q_ref[...] = jnp.sqrt(total_leaves * leaf / e_ref[:rounds, :1])


def local(prior_basis, samples):
    rounds, rows, columns = samples.shape
    basis = prior_basis.shape[1]
    total = rounds * columns
    packed = LANES * len(blocks(total, basis))
    tile = min(TILE, rows)
    leaves = rows // LEAF
    total_leaves = leaves * lax.axis_size("row")
    grid = (rows // tile,)
    p_spec = pl.BlockSpec((tile, basis), lambda i: (i, 0))
    samples = jnp.swapaxes(samples, 1, 2)
    s_spec = pl.BlockSpec((rounds, columns, tile), lambda i: (0, 0, i))
    whole = lambda *shape: pl.BlockSpec(shape, lambda i: (0,) * len(shape))
    part = pl.pallas_call(
        stats_kernel,
        grid=grid,
        in_specs=[p_spec, s_spec],
        out_specs=whole(packed, LANES),
        out_shape=jax.ShapeDtypeStruct((packed, LANES), F32),
        name="stats",
    )(prior_basis, samples)
    stat = all_sum(part)
    w, lt, energy = pl.pallas_call(
        functools.partial(factor_kernel, columns),
        out_shape=(
            jax.ShapeDtypeStruct((total, basis + total), F32),
            jax.ShapeDtypeStruct((total, total), F32),
            jax.ShapeDtypeStruct((8, 128), F32),
        ),
        scratch_shapes=[pltpu.VMEM((total, 2 * total), F32)],
        name="factor",
    )(stat)
    return pl.pallas_call(
        functools.partial(final_kernel, total_leaves, columns),
        grid=grid,
        in_specs=[p_spec, s_spec, whole(total, basis + total), whole(total, total), whole(8, 128)],
        out_specs=(pl.BlockSpec((tile, total), lambda i: (i, 0)), whole(rounds, leaves)),
        out_shape=(
            jax.ShapeDtypeStruct((rows, total), F32),
            jax.ShapeDtypeStruct((rounds, leaves), F32),
        ),
        scratch_shapes=[
            pltpu.VMEM((total, basis + total), BF16),
            pltpu.VMEM((total, basis + total), BF16),
            pltpu.VMEM((total, total), BF16),
            pltpu.VMEM((total, total), BF16),
            pltpu.VMEM((leaves, total), F32),
        ],
        name="final",
    )(prior_basis, samples, w, lt, energy)


def solution(mesh):
    in_specs = (P(("grp", "row"), None), P(None, ("grp", "row"), None))
    out_specs = (P(("grp", "row"), None), P(None, ("grp", "row")))
    return jax.shard_map(local, mesh=mesh, in_specs=in_specs, out_specs=out_specs, check_vma=False)
```

```python
import functools

import jax
import jax.numpy as jnp
from jax import lax
from jax.experimental import pallas as pl
from jax.experimental.pallas import tpu as pltpu
from jax.sharding import PartitionSpec as P

LEAF = 256
LANES = 128
TILE = 512
F32 = jnp.float32
BF16 = jnp.bfloat16
MESH = pl.DeviceIdType.MESH
NN = (((1,), (0,)), ((), ()))
NT = (((1,), (1,)), ((), ()))
TN = (((0,), (0,)), ((), ()))


def split(x):
    hi = x.astype(BF16)
    return hi, (x - hi.astype(F32)).astype(BF16)


def dot(a, b, dims=NN):
    return lax.dot_general(a, b, dims, preferred_element_type=F32)


def exact(a, b, dims=NN):
    return lax.dot_general(
        a, b, dims, precision=lax.Precision.HIGHEST, preferred_element_type=F32
    )


def blocks(total, basis):
    n, b = total // LANES, basis // LANES
    return [(i, j) for i in range(n) for j in range(b)] + [
        (i, b + j) for i in range(n) for j in range(i + 1)
    ]


def unpack(x_ref, total, basis):
    place = {k: i for i, k in enumerate(blocks(total, basis))}
    n, b = total // LANES, basis // LANES

    def block(i, j):
        if j >= b and j - b > i:
            return block(j - b, b + i).T
        k = place[i, j]
        return x_ref[k * LANES : (k + 1) * LANES, :]

    full = [[block(i, j) for j in range(b + n)] for i in range(n)]
    rows = [jnp.concatenate(line, axis=1) for line in full]
    out = jnp.concatenate(rows, axis=0)
    return out[:, :basis], out[:, basis:]


def stats_kernel(p_ref, s_ref, o_ref):
    rounds, columns = s_ref.shape[:2]
    basis = p_ref.shape[1]

    @pl.when(pl.program_id(0) == 0)
    def _():
        o_ref[...] = jnp.zeros_like(o_ref)

    st = jnp.concatenate([s_ref[r] for r in range(rounds)], axis=0)
    sh, sl = split(st)
    ph, plo = split(p_ref[...])
    c = dot(sh, ph) + dot(sl, ph) + dot(sh, plo)
    g = dot(sh, sh, NT) + dot(sl, sh, NT) + dot(sh, sl, NT)
    x = jnp.concatenate([c, g], axis=1)
    for k, (i, j) in enumerate(blocks(rounds * columns, basis)):
        o_ref[k * LANES : (k + 1) * LANES, :] += x[
            i * LANES : (i + 1) * LANES, j * LANES : (j + 1) * LANES
        ]


def sum_kernel(line, x_ref, o_ref, pair, mine, theirs, beside, ready, got, total, pair_send, pair_recv, y_send, y_recv, z_send, z_recv, oz_send, oz_recv, oy_send, oy_recv, oc_send, oc_recv):
    me = lax.axis_index("row")
    core = lax.rem(me, 2)
    y = lax.rem(me // 2, 2)
    z = me // 4
    mate = me + 1 - 2 * core
    next_y = me + 2 - 4 * y
    offsets = sorted(range(1, line), key=lambda i: abs(i - line // 2))
    peers = [lax.rem(z + i, line) for i in offsets]
    order = peers + [z]

    def device(t):
        return 4 * t + 2 * y + core

    barrier = pltpu.get_barrier_semaphore()
    for other in [mate, next_y] + [device(t) for t in peers]:
        pl.semaphore_signal(barrier, inc=1, device_id={"row": other}, device_id_type=MESH)
    pl.semaphore_wait(barrier, line + 1)

    started = []

    def send(src, dst, send_sem, recv_sem, other):
        c = pltpu.make_async_remote_copy(
            src_ref=src, dst_ref=dst, send_sem=send_sem, recv_sem=recv_sem,
            device_id={"row": other}, device_id_type=MESH,
        )
        c.start()
        started.append(c)

    def arrived(block, recv_sem):
        pltpu.make_async_copy(block, block, recv_sem).wait()

    for t in order:
        send(x_ref.at[1 - core, :, t], pair.at[:, t], pair_send.at[t], pair_recv.at[t], mate)
    for t in order:
        arrived(pair.at[:, t], pair_recv.at[t])
        theirs[t] = x_ref[core, 1 - y, t] + pair[1 - y, t]
        mine[t] = x_ref[core, y, t] + pair[y, t]
        send(theirs.at[t], beside.at[t], y_send.at[t], y_recv.at[t], next_y)
    for t in peers:
        arrived(beside.at[t], y_recv.at[t])
        ready[t] = mine[t] + beside[t]
        send(ready.at[t], got.at[z], z_send.at[t], z_recv.at[z], device(t))
    arrived(beside.at[z], y_recv.at[z])
    value = mine[z] + beside[z]
    for t in reversed(peers):
        arrived(got.at[t], z_recv.at[t])
        value = value + got[t]
    total[...] = value
    home = o_ref.at[core, y, z]
    o_ref[core, y, z] = value
    for t in peers:
        send(total, home, oz_send.at[t], oz_recv.at[z], device(t))
    send(total, home, oy_send.at[z], oy_recv.at[z], next_y)
    send(total, home, oc_send.at[y, z], oc_recv.at[y, z], mate)
    back = [z] + list(reversed(peers))
    for i, t in enumerate(back):
        if i:
            block = o_ref.at[core, y, t]
            arrived(block, oz_recv.at[t])
            send(block, block, oy_send.at[t], oy_recv.at[t], next_y)
            send(block, block, oc_send.at[y, t], oc_recv.at[y, t], mate)
    for t in back:
        block = o_ref.at[core, 1 - y, t]
        arrived(block, oy_recv.at[t])
        send(block, block, oc_send.at[1 - y, t], oc_recv.at[1 - y, t], mate)
    for t in back:
        for side in range(2):
            arrived(o_ref.at[1 - core, side, t], oc_recv.at[side, t])
    for c in started:
        c.wait_send()


def all_sum(x):
    n = lax.axis_size("row")
    line = n // 4
    rows, width = x.shape
    chunk = (rows // n, width)
    vmem = pl.BlockSpec(memory_space=pltpu.VMEM)
    sem = pltpu.SemaphoreType.DMA
    out = pl.pallas_call(
        functools.partial(sum_kernel, line),
        in_specs=[vmem],
        out_specs=vmem,
        out_shape=jax.ShapeDtypeStruct((2, 2, line) + chunk, F32),
        scratch_shapes=[pltpu.VMEM((2, line) + chunk, F32)]
        + [pltpu.VMEM((line,) + chunk, F32)] * 5
        + [pltpu.VMEM(chunk, F32)]
        + [sem((line,))] * 10
        + [sem((2, line))] * 2,
        compiler_params=pltpu.CompilerParams(collective_id=0, has_side_effects=True),
        name="all_sum",
    )(x.reshape((2, 2, line) + chunk))
    return out.reshape(rows, width)


def factor_block(block):
    size = block.shape[0]
    width = 2 * size
    groups = size // 8
    eye = (
        lax.broadcasted_iota(jnp.int32, (size, size), 0)
        == lax.broadcasted_iota(jnp.int32, (size, size), 1)
    ).astype(F32)
    aug = jnp.concatenate([block, eye], axis=1)
    rows = [aug[8 * g : 8 * g + 8, :] for g in range(groups)]
    sub = lax.broadcasted_iota(jnp.int32, (8, width), 0)
    for p in range(groups):
        cols = {
            g: [
                jnp.broadcast_to(rows[g][:, 8 * p + j : 8 * p + j + 1], (8, width))
                for j in range(8)
            ]
            for g in range(p, groups)
        }
        v = rows[p]
        scale = jnp.zeros((8, width), F32)
        scaled = []
        for k in range(8):
            d = cols[p][k][k : k + 1, :]
            rinv = 1.0 / d
            scale = jnp.where(sub == k, jnp.broadcast_to(lax.rsqrt(d), (8, width)), scale)
            vk = v[k : k + 1, :] * rinv
            scaled.append(vk)
            below = jnp.where(sub > k, cols[p][k], 0.0)
            steps = {j: cols[p][j][k : k + 1, :] * rinv for j in range(k + 1, 8)}
            for j in range(k + 1, 8):
                cols[p][j] = cols[p][j] - below * steps[j]
            v = v - below * vk
            for g in range(p + 1, groups):
                for j in range(k + 1, 8):
                    cols[g][j] = cols[g][j] - cols[g][k] * steps[j]
        for g in range(p + 1, groups):
            for k in range(8):
                rows[g] = rows[g] - cols[g][k] * scaled[k]
        rows[p] = v * scale
    return jnp.concatenate(rows, axis=0)


def finish_kernel(columns, total_leaves, x_ref, p_hbm, s_hbm, n_hbm, q_ref, p_v, s_v, n_v, ae_ref, lt_ref, xs, ns, wh, wl, lh, ll, sums, p_sem, s_sem, n_sem):
    total = lt_ref.shape[0]
    rows, basis = p_v.shape
    rounds = total // columns
    tile = ns.shape[1]
    chunks = rows // tile
    depth = basis + total

    def at(i):
        return slice(i * tile, (i + 1) * tile)

    loads = []
    for i in range(chunks):
        loads.append(pltpu.make_async_copy(p_hbm.at[at(i)], p_v.at[at(i)], p_sem.at[i]))
        loads.append(pltpu.make_async_copy(s_hbm.at[:, :, at(i)], s_v.at[:, :, at(i)], s_sem.at[i]))
    for c in loads:
        c.start()

    ct, g = unpack(x_ref, total, basis)
    row = lax.broadcasted_iota(jnp.int32, (total, total), 0)
    col = lax.broadcasted_iota(jnp.int32, (total, total), 1)
    eye = row == col
    diag = jnp.sum(jnp.where(eye, g, 0.0), axis=1, keepdims=True)
    energy = jnp.concatenate(
        [
            jnp.sum(diag[r * columns : (r + 1) * columns, :], axis=0, keepdims=True)
            for r in range(rounds)
        ],
        axis=0,
    )
    ae_ref[:, :total] = g - exact(ct, ct, NT)
    ae_ref[:, total:] = eye.astype(F32)
    lt_ref[...] = jnp.zeros_like(lt_ref)
    upper = (
        lax.broadcasted_iota(jnp.int32, (columns, columns), 0)
        <= lax.broadcasted_iota(jnp.int32, (columns, columns), 1)
    )
    for r in range(rounds):
        lo, hi = r * columns, (r + 1) * columns
        both = factor_block(ae_ref[lo:hi, lo:hi])
        lt_ref[lo:hi, lo:hi] = jnp.where(upper, both[:, :columns], 0.0)
        z = exact(both[:, columns:], ae_ref[lo:hi, :])
        ae_ref[lo:hi, :] = z
        if r + 1 < rounds:
            ae_ref[hi:, :] -= exact(z[:, hi:total], z, TN)
    linv = ae_ref[:, total:]
    wh[:basis], wl[:basis] = split(-exact(linv, ct).T)
    wh[basis:], wl[basis:] = split(linv.T)
    lh[...], ll[...] = split(lt_ref[...])
    for c in loads:
        c.wait()

    def prepare(i):
        slot = i % 2
        h, l = split(p_v[at(i), :])
        xs[slot, :, :basis] = h
        xs[slot, :, depth : depth + basis] = l
        h, l = split(jnp.concatenate([s_v[r, :, at(i)] for r in range(rounds)], axis=0).T)
        xs[slot, :, basis:depth] = h
        xs[slot, :, depth + basis :] = l

    def product(i):
        slot = i % 2
        h, l = xs[slot, :, :depth], xs[slot, :, depth:]
        out = dot(h, wh[...]) + dot(l, wh[...]) + dot(h, wl[...])
        n_v[at(i), :] = out
        ns[slot, :, :total], ns[slot, :, total:] = split(out)

    def remains(i):
        slot = i % 2
        h, l = ns[slot, :, :total], ns[slot, :, total:]
        rem = dot(h, lh[...]) + dot(l, lh[...]) + dot(h, ll[...])
        sq = rem * rem
        for k in range(tile // LEAF):
            leaf = i * (tile // LEAF) + k
            sums[leaf : leaf + 1, :] = jnp.sum(
                sq[k * LEAF : (k + 1) * LEAF, :], axis=0, keepdims=True
            )

    stores = [
        pltpu.make_async_copy(n_v.at[at(i)], n_hbm.at[at(i)], n_sem.at[i]) for i in range(chunks)
    ]
    prepare(0)
    for i in range(chunks):
        product(i)
        if i + 1 < chunks:
            prepare(i + 1)
        if i:
            stores[i - 1].start()
            remains(i - 1)
    stores[-1].start()
    remains(chunks - 1)
    pick = (
        lax.broadcasted_iota(jnp.int32, (rounds, total), 1) // columns
        == lax.broadcasted_iota(jnp.int32, (rounds, total), 0)
    ).astype(F32)
    q_ref[...] = jnp.sqrt(total_leaves * exact(pick, sums[...], NT) / energy)
    for c in stores:
        c.wait()


def local(prior_basis, samples):
    rounds, rows, columns = samples.shape
    basis = prior_basis.shape[1]
    total = rounds * columns
    packed = LANES * len(blocks(total, basis))
    tile = min(1024, rows)
    leaves = rows // LEAF
    total_leaves = leaves * lax.axis_size("row")
    samples = jnp.swapaxes(samples, 1, 2)
    part = pl.pallas_call(
        stats_kernel,
        grid=(rows // tile,),
        in_specs=[
            pl.BlockSpec((tile, basis), lambda i: (i, 0)),
            pl.BlockSpec((rounds, columns, tile), lambda i: (0, 0, i)),
        ],
        out_specs=pl.BlockSpec((packed, LANES), lambda i: (0, 0)),
        out_shape=jax.ShapeDtypeStruct((packed, LANES), F32),
        name="stats",
    )(prior_basis, samples)
    stat = all_sum(part)
    depth = basis + total
    chunk = min(TILE, rows)
    vmem = pl.BlockSpec(memory_space=pltpu.VMEM)
    hbm = pl.BlockSpec(memory_space=pl.ANY)
    sem = pltpu.SemaphoreType.DMA((rows // chunk,))
    return pl.pallas_call(
        functools.partial(finish_kernel, columns, total_leaves),
        in_specs=[vmem, hbm, hbm],
        out_specs=(hbm, vmem),
        out_shape=(
            jax.ShapeDtypeStruct((rows, total), F32),
            jax.ShapeDtypeStruct((rounds, leaves), F32),
        ),
        scratch_shapes=[
            pltpu.VMEM((rows, basis), F32),
            pltpu.VMEM((rounds, columns, rows), F32),
            pltpu.VMEM((rows, total), F32),
            pltpu.VMEM((total, 2 * total), F32),
            pltpu.VMEM((total, total), F32),
            pltpu.VMEM((2, chunk, 2 * depth), BF16),
            pltpu.VMEM((2, chunk, 2 * total), BF16),
            pltpu.VMEM((depth, total), BF16),
            pltpu.VMEM((depth, total), BF16),
            pltpu.VMEM((total, total), BF16),
            pltpu.VMEM((total, total), BF16),
            pltpu.VMEM((leaves, total), F32),
            sem,
            sem,
            sem,
        ],
        name="finish",
    )(stat, prior_basis, samples)


def solution(mesh):
    in_specs = (P(("grp", "row"), None), P(None, ("grp", "row"), None))
    out_specs = (P(("grp", "row"), None), P(None, ("grp", "row")))
    return jax.shard_map(local, mesh=mesh, in_specs=in_specs, out_specs=out_specs, check_vma=False)
```

```python
import functools

import jax
import jax.numpy as jnp
from jax import lax
from jax.experimental import pallas as pl
from jax.experimental.pallas import tpu as pltpu
from jax.sharding import PartitionSpec as P

LEAF = 256
LANES = 128
TILE = 512
F32 = jnp.float32
BF16 = jnp.bfloat16
MESH = pl.DeviceIdType.MESH
NN = (((1,), (0,)), ((), ()))
NT = (((1,), (1,)), ((), ()))
TN = (((0,), (0,)), ((), ()))


def split(x):
    hi = x.astype(BF16)
    return hi, (x - hi.astype(F32)).astype(BF16)


def dot(a, b, dims=NN):
    return lax.dot_general(a, b, dims, preferred_element_type=F32)


def exact(a, b, dims=NN):
    return lax.dot_general(
        a, b, dims, precision=lax.Precision.HIGHEST, preferred_element_type=F32
    )


def blocks(total, basis):
    n, b = total // LANES, basis // LANES
    return [(i, j) for i in range(n) for j in range(b)] + [
        (i, b + j) for i in range(n) for j in range(i + 1)
    ]


def unpack(x_ref, total, basis):
    place = {k: i for i, k in enumerate(blocks(total, basis))}
    n, b = total // LANES, basis // LANES

    def block(i, j):
        if j >= b and j - b > i:
            return block(j - b, b + i).T
        k = place[i, j]
        return x_ref[k * LANES : (k + 1) * LANES, :]

    full = [[block(i, j) for j in range(b + n)] for i in range(n)]
    rows = [jnp.concatenate(line, axis=1) for line in full]
    out = jnp.concatenate(rows, axis=0)
    return out[:, :basis], out[:, basis:]


def sum_kernel(line, p_hbm, s_hbm, o_ref, p_v, s_v, ph, plo, st, acc, x_ref, p_sem, s_sem, pair, mine, theirs, beside, ready, got, total, pair_send, pair_recv, y_send, y_recv, z_send, z_recv, oz_send, oz_recv, oy_send, oy_recv, oc_send, oc_recv):
    me = lax.axis_index("row")
    core = lax.rem(me, 2)
    y = lax.rem(me // 2, 2)
    z = me // 4
    mate = me + 1 - 2 * core
    next_y = me + 2 - 4 * y
    offsets = sorted(range(1, line), key=lambda i: abs(i - line // 2))
    peers = [lax.rem(z + i, line) for i in offsets]
    order = peers + [z]

    def device(t):
        return 4 * t + 2 * y + core

    barrier = pltpu.get_barrier_semaphore()
    for other in [mate, next_y] + [device(t) for t in peers]:
        pl.semaphore_signal(barrier, inc=1, device_id={"row": other}, device_id_type=MESH)
    rows, basis = p_v.shape
    rounds, columns = s_v.shape[:2]
    width = rounds * columns
    tile = ph.shape[1]
    tiles = rows // tile

    def at(i):
        return slice(i * tile, (i + 1) * tile)

    loads = [
        (
            pltpu.make_async_copy(p_hbm.at[at(i)], p_v.at[at(i)], p_sem.at[i]),
            pltpu.make_async_copy(s_hbm.at[:, :, at(i)], s_v.at[:, :, at(i)], s_sem.at[i]),
        )
        for i in range(tiles)
    ]
    for one, two in loads:
        one.start()
        two.start()

    def prepare(i):
        slot = i % 2
        for c in loads[i]:
            c.wait()
        ph[slot], plo[slot] = split(p_v[at(i), :])
        rows_of = jnp.concatenate([s_v[r, :, at(i)] for r in range(rounds)], axis=0)
        st[slot, :width], st[slot, width:] = split(rows_of)

    prepare(0)
    for i in range(tiles):
        slot = i % 2
        sh, sl = st[slot, :width], st[slot, width:]
        c = dot(sh, ph[slot]) + dot(sl, ph[slot]) + dot(sh, plo[slot])
        g = dot(sh, sh, NT) + dot(sl, sh, NT) + dot(sh, sl, NT)
        if i + 1 < tiles:
            prepare(i + 1)
        if i:
            acc[:, :basis] += c
            acc[:, basis:] += g
        else:
            acc[:, :basis] = c
            acc[:, basis:] = g
    high = x_ref.shape[-2]
    for k, (i, j) in enumerate(blocks(width, basis)):
        first, end = k * LANES, (k + 1) * LANES
        while first < end:
            slot, inside = divmod(first, high)
            count = min(high - inside, end - first)
            source = i * LANES + first - k * LANES
            x_ref[
                slot // (2 * line), slot // line % 2, slot % line, inside : inside + count, :
            ] = acc[source : source + count, j * LANES : (j + 1) * LANES]
            first += count

    pl.semaphore_wait(barrier, line + 1)
    started = []

    def send(src, dst, send_sem, recv_sem, other):
        c = pltpu.make_async_remote_copy(
            src_ref=src, dst_ref=dst, send_sem=send_sem, recv_sem=recv_sem,
            device_id={"row": other}, device_id_type=MESH,
        )
        c.start()
        started.append(c)

    def arrived(block, recv_sem):
        pltpu.make_async_copy(block, block, recv_sem).wait()

    for t in order:
        send(x_ref.at[1 - core, :, t], pair.at[:, t], pair_send.at[t], pair_recv.at[t], mate)
    for t in order:
        arrived(pair.at[:, t], pair_recv.at[t])
        theirs[t] = x_ref[core, 1 - y, t] + pair[1 - y, t]
        mine[t] = x_ref[core, y, t] + pair[y, t]
        send(theirs.at[t], beside.at[t], y_send.at[t], y_recv.at[t], next_y)
    for t in peers:
        arrived(beside.at[t], y_recv.at[t])
        ready[t] = mine[t] + beside[t]
        send(ready.at[t], got.at[z], z_send.at[t], z_recv.at[z], device(t))
    arrived(beside.at[z], y_recv.at[z])
    value = mine[z] + beside[z]
    for t in reversed(peers):
        arrived(got.at[t], z_recv.at[t])
        value = value + got[t]
    total[...] = value
    home = o_ref.at[core, y, z]
    o_ref[core, y, z] = value
    for t in peers:
        send(total, home, oz_send.at[t], oz_recv.at[z], device(t))
    send(total, home, oy_send.at[z], oy_recv.at[z], next_y)
    send(total, home, oc_send.at[y, z], oc_recv.at[y, z], mate)
    back = [z] + list(reversed(peers))
    for i, t in enumerate(back):
        if i:
            block = o_ref.at[core, y, t]
            arrived(block, oz_recv.at[t])
            send(block, block, oy_send.at[t], oy_recv.at[t], next_y)
            send(block, block, oc_send.at[y, t], oc_recv.at[y, t], mate)
    for t in back:
        block = o_ref.at[core, 1 - y, t]
        arrived(block, oy_recv.at[t])
        send(block, block, oc_send.at[1 - y, t], oc_recv.at[1 - y, t], mate)
    for t in back:
        for side in range(2):
            arrived(o_ref.at[1 - core, side, t], oc_recv.at[side, t])
    for c in started:
        c.wait_send()


def all_sum(prior_basis, samples):
    n = lax.axis_size("row")
    line = n // 4
    rounds, columns, rows = samples.shape
    basis = prior_basis.shape[1]
    total = rounds * columns
    packed = LANES * len(blocks(total, basis))
    chunk = (packed // n, LANES)
    tile = min(TILE, rows)
    hbm = pl.BlockSpec(memory_space=pl.ANY)
    sem = pltpu.SemaphoreType.DMA
    out = pl.pallas_call(
        functools.partial(sum_kernel, line),
        in_specs=[hbm, hbm],
        out_specs=pl.BlockSpec(memory_space=pltpu.VMEM),
        out_shape=jax.ShapeDtypeStruct((2, 2, line) + chunk, F32),
        scratch_shapes=[
            pltpu.VMEM((rows, basis), F32),
            pltpu.VMEM((rounds, columns, rows), F32),
            pltpu.VMEM((2, tile, basis), BF16),
            pltpu.VMEM((2, tile, basis), BF16),
            pltpu.VMEM((2, 2 * total, tile), BF16),
            pltpu.VMEM((total, basis + total), F32),
            pltpu.VMEM((2, 2, line) + chunk, F32),
            sem((rows // tile,)),
            sem((rows // tile,)),
            pltpu.VMEM((2, line) + chunk, F32),
        ]
        + [pltpu.VMEM((line,) + chunk, F32)] * 5
        + [pltpu.VMEM(chunk, F32)]
        + [sem((line,))] * 10
        + [sem((2, line))] * 2,
        compiler_params=pltpu.CompilerParams(collective_id=0, has_side_effects=True),
        name="all_sum",
    )(prior_basis, samples)
    return out.reshape(packed, LANES)


def factor_block(block):
    size = block.shape[0]
    width = 2 * size
    groups = size // 8
    eye = (
        lax.broadcasted_iota(jnp.int32, (size, size), 0)
        == lax.broadcasted_iota(jnp.int32, (size, size), 1)
    ).astype(F32)
    aug = jnp.concatenate([block, eye], axis=1)
    rows = [aug[8 * g : 8 * g + 8, :] for g in range(groups)]
    sub = lax.broadcasted_iota(jnp.int32, (8, width), 0)
    for p in range(groups):
        cols = {
            g: [
                jnp.broadcast_to(rows[g][:, 8 * p + j : 8 * p + j + 1], (8, width))
                for j in range(8)
            ]
            for g in range(p, groups)
        }
        v = rows[p]
        scale = jnp.zeros((8, width), F32)
        scaled = []
        for k in range(8):
            spread = lambda x: jnp.broadcast_to(x[k : k + 1, :], (8, width))
            d = spread(cols[p][k])
            rinv = 1.0 / d
            scale = jnp.where(sub == k, lax.rsqrt(d), scale)
            below = jnp.where(sub > k, cols[p][k], 0.0)
            heads = {j: spread(cols[p][j]) for j in range(k + 1, 8)}
            terms = {j: below * heads[j] for j in heads}
            head = spread(v)
            term = below * head
            for j in heads:
                cols[p][j] = cols[p][j] - terms[j] * rinv
            v = v - term * rinv
            scaled.append(head * rinv)
            for g in range(p + 1, groups):
                ratio = cols[g][k] * rinv
                for j in heads:
                    cols[g][j] = cols[g][j] - ratio * heads[j]
        for g in range(p + 1, groups):
            for k in range(8):
                rows[g] = rows[g] - cols[g][k] * scaled[k]
        rows[p] = v * scale
    return jnp.concatenate(rows, axis=0)


def finish_kernel(columns, total_leaves, x_ref, p_hbm, s_hbm, n_hbm, q_ref, p_v, s_v, n_v, ae_ref, lt_ref, xs, ns, wh, wl, lh, ll, sums, p_sem, s_sem, n_sem):
    total = lt_ref.shape[0]
    rows, basis = p_v.shape
    rounds = total // columns
    tile = ns.shape[1]
    chunks = rows // tile
    depth = basis + total

    def at(i):
        return slice(i * tile, (i + 1) * tile)

    loads = []
    for i in range(chunks):
        loads.append(pltpu.make_async_copy(p_hbm.at[at(i)], p_v.at[at(i)], p_sem.at[i]))
        loads.append(pltpu.make_async_copy(s_hbm.at[:, :, at(i)], s_v.at[:, :, at(i)], s_sem.at[i]))
    for c in loads:
        c.start()

    ct, g = unpack(x_ref, total, basis)
    row = lax.broadcasted_iota(jnp.int32, (total, total), 0)
    col = lax.broadcasted_iota(jnp.int32, (total, total), 1)
    eye = row == col
    diag = jnp.sum(jnp.where(eye, g, 0.0), axis=1, keepdims=True)
    energy = jnp.concatenate(
        [
            jnp.sum(diag[r * columns : (r + 1) * columns, :], axis=0, keepdims=True)
            for r in range(rounds)
        ],
        axis=0,
    )
    ae_ref[:, :total] = g - exact(ct, ct, NT)
    ae_ref[:, total:] = eye.astype(F32)
    lt_ref[...] = jnp.zeros_like(lt_ref)
    upper = (
        lax.broadcasted_iota(jnp.int32, (columns, columns), 0)
        <= lax.broadcasted_iota(jnp.int32, (columns, columns), 1)
    )
    for r in range(rounds):
        lo, hi = r * columns, (r + 1) * columns
        both = factor_block(ae_ref[lo:hi, lo:hi])
        lt_ref[lo:hi, lo:hi] = jnp.where(upper, both[:, :columns], 0.0)
        z = exact(both[:, columns:], ae_ref[lo:hi, :])
        ae_ref[lo:hi, :] = z
        if r + 1 < rounds:
            ae_ref[hi:, :] -= exact(z[:, hi:total], z, TN)
    linv = ae_ref[:, total:]
    wh[:basis], wl[:basis] = split(-exact(linv, ct).T)
    wh[basis:], wl[basis:] = split(linv.T)
    lh[...], ll[...] = split(lt_ref[...])
    for c in loads:
        c.wait()

    def prepare(i):
        slot = i % 2
        h, l = split(p_v[at(i), :])
        xs[slot, :, :basis] = h
        xs[slot, :, depth : depth + basis] = l
        h, l = split(jnp.concatenate([s_v[r, :, at(i)] for r in range(rounds)], axis=0).T)
        xs[slot, :, basis:depth] = h
        xs[slot, :, depth + basis :] = l

    def product(i):
        slot = i % 2
        h, l = xs[slot, :, :depth], xs[slot, :, depth:]
        out = dot(h, wh[...]) + dot(l, wh[...]) + dot(h, wl[...])
        n_v[at(i), :] = out
        ns[slot, :, :total], ns[slot, :, total:] = split(out)

    def remains(i):
        slot = i % 2
        h, l = ns[slot, :, :total], ns[slot, :, total:]
        rem = dot(h, lh[...]) + dot(l, lh[...]) + dot(h, ll[...])
        sq = rem * rem
        for k in range(tile // LEAF):
            leaf = i * (tile // LEAF) + k
            sums[leaf : leaf + 1, :] = jnp.sum(
                sq[k * LEAF : (k + 1) * LEAF, :], axis=0, keepdims=True
            )

    stores = [
        pltpu.make_async_copy(n_v.at[at(i)], n_hbm.at[at(i)], n_sem.at[i]) for i in range(chunks)
    ]
    prepare(0)
    for i in range(chunks):
        product(i)
        if i + 1 < chunks:
            prepare(i + 1)
        if i:
            stores[i - 1].start()
            remains(i - 1)
    stores[-1].start()
    remains(chunks - 1)
    pick = (
        lax.broadcasted_iota(jnp.int32, (rounds, total), 1) // columns
        == lax.broadcasted_iota(jnp.int32, (rounds, total), 0)
    ).astype(F32)
    q_ref[...] = jnp.sqrt(total_leaves * exact(pick, sums[...], NT) / energy)
    for c in stores:
        c.wait()


def local(prior_basis, samples):
    rounds, rows, columns = samples.shape
    basis = prior_basis.shape[1]
    total = rounds * columns
    leaves = rows // LEAF
    total_leaves = leaves * lax.axis_size("row")
    samples = jnp.swapaxes(samples, 1, 2)
    stat = all_sum(prior_basis, samples)
    depth = basis + total
    chunk = min(TILE, rows)
    vmem = pl.BlockSpec(memory_space=pltpu.VMEM)
    hbm = pl.BlockSpec(memory_space=pl.ANY)
    sem = pltpu.SemaphoreType.DMA((rows // chunk,))
    return pl.pallas_call(
        functools.partial(finish_kernel, columns, total_leaves),
        in_specs=[vmem, hbm, hbm],
        out_specs=(hbm, vmem),
        out_shape=(
            jax.ShapeDtypeStruct((rows, total), F32),
            jax.ShapeDtypeStruct((rounds, leaves), F32),
        ),
        scratch_shapes=[
            pltpu.VMEM((rows, basis), F32),
            pltpu.VMEM((rounds, columns, rows), F32),
            pltpu.VMEM((rows, total), F32),
            pltpu.VMEM((total, 2 * total), F32),
            pltpu.VMEM((total, total), F32),
            pltpu.VMEM((2, chunk, 2 * depth), BF16),
            pltpu.VMEM((2, chunk, 2 * total), BF16),
            pltpu.VMEM((depth, total), BF16),
            pltpu.VMEM((depth, total), BF16),
            pltpu.VMEM((total, total), BF16),
            pltpu.VMEM((total, total), BF16),
            pltpu.VMEM((leaves, total), F32),
            sem,
            sem,
            sem,
        ],
        name="finish",
    )(stat, prior_basis, samples)


def solution(mesh):
    in_specs = (P(("grp", "row"), None), P(None, ("grp", "row"), None))
    out_specs = (P(("grp", "row"), None), P(None, ("grp", "row")))
    return jax.shard_map(local, mesh=mesh, in_specs=in_specs, out_specs=out_specs, check_vma=False)
```

```python
import functools

import jax
import jax.numpy as jnp
from jax import lax
from jax.experimental import pallas as pl
from jax.experimental.pallas import tpu as pltpu
from jax.sharding import PartitionSpec as P

LEAF = 256
LANES = 128
TILE = 512
F32 = jnp.float32
BF16 = jnp.bfloat16
MESH = pl.DeviceIdType.MESH
NN = (((1,), (0,)), ((), ()))
NT = (((1,), (1,)), ((), ()))
TN = (((0,), (0,)), ((), ()))


def split(x):
    hi = x.astype(BF16)
    return hi, (x - hi.astype(F32)).astype(BF16)


def dot(a, b, dims=NN):
    return lax.dot_general(a, b, dims, preferred_element_type=F32)


def exact(a, b, dims=NN):
    return lax.dot_general(
        a, b, dims, precision=lax.Precision.HIGHEST, preferred_element_type=F32
    )


def blocks(total, basis):
    n, b = total // LANES, basis // LANES
    return [(i, j) for i in range(n) for j in range(b)] + [
        (i, b + j) for i in range(n) for j in range(i + 1)
    ]


def unpack(x_ref, total, basis):
    place = {k: i for i, k in enumerate(blocks(total, basis))}
    n, b = total // LANES, basis // LANES

    def block(i, j):
        if j >= b and j - b > i:
            return block(j - b, b + i).T
        k = place[i, j]
        return x_ref[k * LANES : (k + 1) * LANES, :]

    full = [[block(i, j) for j in range(b + n)] for i in range(n)]
    rows = [jnp.concatenate(line, axis=1) for line in full]
    out = jnp.concatenate(rows, axis=0)
    return out[:, :basis], out[:, basis:]


def sum_kernel(line, p_hbm, s_hbm, o_ref, p_v, s_v, ph, plo, st, acc, x_ref, p_sem, s_sem, pair, mine, theirs, beside, ready, got, total, pair_send, pair_recv, y_send, y_recv, z_send, z_recv, oz_send, oz_recv, oy_send, oy_recv, oc_send, oc_recv):
    me = lax.axis_index("row")
    core = lax.rem(me, 2)
    y = lax.rem(me // 2, 2)
    z = me // 4
    mate = me + 1 - 2 * core
    next_y = me + 2 - 4 * y
    offsets = sorted(range(1, line), key=lambda i: abs(i - line // 2))
    peers = [lax.rem(z + i, line) for i in offsets]
    order = peers + [z]

    def device(t):
        return 4 * t + 2 * y + core

    barrier = pltpu.get_barrier_semaphore()
    for other in [mate, next_y] + [device(t) for t in peers]:
        pl.semaphore_signal(barrier, inc=1, device_id={"row": other}, device_id_type=MESH)
    rows, basis = p_v.shape
    rounds, columns = s_v.shape[:2]
    width = rounds * columns
    tile = ph.shape[1]
    tiles = rows // tile

    def at(i):
        return slice(i * tile, (i + 1) * tile)

    loads = [
        (
            pltpu.make_async_copy(p_hbm.at[at(i)], p_v.at[at(i)], p_sem.at[i]),
            pltpu.make_async_copy(s_hbm.at[:, :, at(i)], s_v.at[:, :, at(i)], s_sem.at[i]),
        )
        for i in range(tiles)
    ]
    for one, two in loads:
        one.start()
        two.start()

    def prepare(i):
        slot = i % 2
        for c in loads[i]:
            c.wait()
        ph[slot], plo[slot] = split(p_v[at(i), :])
        rows_of = jnp.concatenate([s_v[r, :, at(i)] for r in range(rounds)], axis=0)
        st[slot, :width], st[slot, width:] = split(rows_of)

    prepare(0)
    for i in range(tiles):
        slot = i % 2
        sh, sl = st[slot, :width], st[slot, width:]
        c = dot(sh, ph[slot]) + dot(sl, ph[slot]) + dot(sh, plo[slot])
        g = dot(sh, sh, NT) + dot(sl, sh, NT) + dot(sh, sl, NT)
        if i + 1 < tiles:
            prepare(i + 1)
        if i:
            acc[:, :basis] += c
            acc[:, basis:] += g
        else:
            acc[:, :basis] = c
            acc[:, basis:] = g
    high = x_ref.shape[-2]
    for k, (i, j) in enumerate(blocks(width, basis)):
        first, end = k * LANES, (k + 1) * LANES
        while first < end:
            slot, inside = divmod(first, high)
            count = min(high - inside, end - first)
            source = i * LANES + first - k * LANES
            x_ref[
                slot // (2 * line), slot // line % 2, slot % line, inside : inside + count, :
            ] = acc[source : source + count, j * LANES : (j + 1) * LANES]
            first += count

    pl.semaphore_wait(barrier, line + 1)
    started = []

    def send(src, dst, send_sem, recv_sem, other):
        c = pltpu.make_async_remote_copy(
            src_ref=src, dst_ref=dst, send_sem=send_sem, recv_sem=recv_sem,
            device_id={"row": other}, device_id_type=MESH,
        )
        c.start()
        started.append(c)

    def arrived(block, recv_sem):
        pltpu.make_async_copy(block, block, recv_sem).wait()

    for t in order:
        send(x_ref.at[1 - core, :, t], pair.at[:, t], pair_send.at[t], pair_recv.at[t], mate)
    for t in order:
        arrived(pair.at[:, t], pair_recv.at[t])
        theirs[t] = x_ref[core, 1 - y, t] + pair[1 - y, t]
        mine[t] = x_ref[core, y, t] + pair[y, t]
        send(theirs.at[t], beside.at[t], y_send.at[t], y_recv.at[t], next_y)
    for t in peers:
        arrived(beside.at[t], y_recv.at[t])
        ready[t] = mine[t] + beside[t]
        send(ready.at[t], got.at[z], z_send.at[t], z_recv.at[z], device(t))
    arrived(beside.at[z], y_recv.at[z])
    value = mine[z] + beside[z]
    for t in reversed(peers):
        arrived(got.at[t], z_recv.at[t])
        value = value + got[t]
    total[...] = value
    home = o_ref.at[core, y, z]
    o_ref[core, y, z] = value
    for t in peers:
        send(total, home, oz_send.at[t], oz_recv.at[z], device(t))
    send(total, home, oy_send.at[z], oy_recv.at[z], next_y)
    send(total, home, oc_send.at[y, z], oc_recv.at[y, z], mate)
    back = [z] + list(reversed(peers))
    for i, t in enumerate(back):
        if i:
            block = o_ref.at[core, y, t]
            arrived(block, oz_recv.at[t])
            send(block, block, oy_send.at[t], oy_recv.at[t], next_y)
            send(block, block, oc_send.at[y, t], oc_recv.at[y, t], mate)
    for t in back:
        block = o_ref.at[core, 1 - y, t]
        arrived(block, oy_recv.at[t])
        send(block, block, oc_send.at[1 - y, t], oc_recv.at[1 - y, t], mate)
    for t in back:
        for side in range(2):
            arrived(o_ref.at[1 - core, side, t], oc_recv.at[side, t])
    for c in started:
        c.wait_send()


def all_sum(prior_basis, samples):
    n = lax.axis_size("row")
    line = n // 4
    rounds, columns, rows = samples.shape
    basis = prior_basis.shape[1]
    total = rounds * columns
    packed = LANES * len(blocks(total, basis))
    chunk = (packed // n, LANES)
    tile = min(TILE, rows)
    hbm = pl.BlockSpec(memory_space=pl.ANY)
    sem = pltpu.SemaphoreType.DMA
    out = pl.pallas_call(
        functools.partial(sum_kernel, line),
        in_specs=[hbm, hbm],
        out_specs=pl.BlockSpec(memory_space=pltpu.VMEM),
        out_shape=jax.ShapeDtypeStruct((2, 2, line) + chunk, F32),
        scratch_shapes=[
            pltpu.VMEM((rows, basis), F32),
            pltpu.VMEM((rounds, columns, rows), F32),
            pltpu.VMEM((2, tile, basis), BF16),
            pltpu.VMEM((2, tile, basis), BF16),
            pltpu.VMEM((2, 2 * total, tile), BF16),
            pltpu.VMEM((total, basis + total), F32),
            pltpu.VMEM((2, 2, line) + chunk, F32),
            sem((rows // tile,)),
            sem((rows // tile,)),
            pltpu.VMEM((2, line) + chunk, F32),
        ]
        + [pltpu.VMEM((line,) + chunk, F32)] * 5
        + [pltpu.VMEM(chunk, F32)]
        + [sem((line,))] * 10
        + [sem((2, line))] * 2,
        compiler_params=pltpu.CompilerParams(collective_id=0, has_side_effects=True),
        name="all_sum",
    )(prior_basis, samples)
    return out.reshape(packed, LANES)


def factor_block(block):
    size = block.shape[0]
    width = 2 * size
    groups = size // 8
    eye = (
        lax.broadcasted_iota(jnp.int32, (size, size), 0)
        == lax.broadcasted_iota(jnp.int32, (size, size), 1)
    ).astype(F32)
    aug = jnp.concatenate([block, eye], axis=1)
    rows = [aug[8 * g : 8 * g + 8, :] for g in range(groups)]
    sub = lax.broadcasted_iota(jnp.int32, (8, width), 0)
    for p in range(groups):
        cols = {
            g: [
                jnp.broadcast_to(rows[g][:, 8 * p + j : 8 * p + j + 1], (8, width))
                for j in range(8)
            ]
            for g in range(p, groups)
        }
        v = rows[p]
        scale = jnp.zeros((8, width), F32)
        scaled = []
        for k in range(8):
            d = cols[p][k][k : k + 1, :]
            rinv = 1.0 / d
            scale = jnp.where(sub == k, jnp.broadcast_to(lax.rsqrt(d), (8, width)), scale)
            vk = v[k : k + 1, :] * rinv
            scaled.append(vk)
            below = jnp.where(sub > k, cols[p][k], 0.0)
            steps = {j: cols[p][j][k : k + 1, :] * rinv for j in range(k + 1, 8)}
            for j in range(k + 1, 8):
                cols[p][j] = cols[p][j] - below * steps[j]
            v = v - below * vk
            for g in range(p + 1, groups):
                for j in range(k + 1, 8):
                    cols[g][j] = cols[g][j] - cols[g][k] * steps[j]
        for g in range(p + 1, groups):
            for k in range(8):
                rows[g] = rows[g] - cols[g][k] * scaled[k]
        rows[p] = v * scale
    return jnp.concatenate(rows, axis=0)


def finish_kernel(columns, total_leaves, x_ref, p_hbm, s_hbm, n_hbm, q_ref, p_v, s_v, n_v, ae_ref, lt_ref, xs, ns, wh, wl, lh, ll, sums, p_sem, s_sem, n_sem):
    total = lt_ref.shape[0]
    rows, basis = p_v.shape
    rounds = total // columns
    tile = ns.shape[1]
    chunks = rows // tile
    depth = basis + total

    def at(i):
        return slice(i * tile, (i + 1) * tile)

    loads = []
    for i in range(chunks):
        loads.append(pltpu.make_async_copy(p_hbm.at[at(i)], p_v.at[at(i)], p_sem.at[i]))
        loads.append(pltpu.make_async_copy(s_hbm.at[:, :, at(i)], s_v.at[:, :, at(i)], s_sem.at[i]))
    for c in loads:
        c.start()

    ct, g = unpack(x_ref, total, basis)
    row = lax.broadcasted_iota(jnp.int32, (total, total), 0)
    col = lax.broadcasted_iota(jnp.int32, (total, total), 1)
    eye = row == col
    diag = jnp.sum(jnp.where(eye, g, 0.0), axis=1, keepdims=True)
    energy = jnp.concatenate(
        [
            jnp.sum(diag[r * columns : (r + 1) * columns, :], axis=0, keepdims=True)
            for r in range(rounds)
        ],
        axis=0,
    )
    ae_ref[:, :total] = g - exact(ct, ct, NT)
    ae_ref[:, total:] = eye.astype(F32)
    lt_ref[...] = jnp.zeros_like(lt_ref)
    upper = (
        lax.broadcasted_iota(jnp.int32, (columns, columns), 0)
        <= lax.broadcasted_iota(jnp.int32, (columns, columns), 1)
    )
    for r in range(rounds):
        lo, hi = r * columns, (r + 1) * columns
        both = factor_block(ae_ref[lo:hi, lo:hi])
        lt_ref[lo:hi, lo:hi] = jnp.where(upper, both[:, :columns], 0.0)
        z = exact(both[:, columns:], ae_ref[lo:hi, :])
        ae_ref[lo:hi, :] = z
        if r + 1 < rounds:
            ae_ref[hi:, :] -= exact(z[:, hi:total], z, TN)
    linv = ae_ref[:, total:]
    wh[:basis], wl[:basis] = split(-exact(linv, ct).T)
    wh[basis:], wl[basis:] = split(linv.T)
    lh[...], ll[...] = split(lt_ref[...])
    for c in loads:
        c.wait()

    def prepare(i):
        slot = i % 2
        h, l = split(p_v[at(i), :])
        xs[slot, :, :basis] = h
        xs[slot, :, depth : depth + basis] = l
        h, l = split(jnp.concatenate([s_v[r, :, at(i)] for r in range(rounds)], axis=0).T)
        xs[slot, :, basis:depth] = h
        xs[slot, :, depth + basis :] = l

    def product(i):
        slot = i % 2
        h, l = xs[slot, :, :depth], xs[slot, :, depth:]
        out = dot(h, wh[...]) + dot(l, wh[...]) + dot(h, wl[...])
        n_v[at(i), :] = out
        ns[slot, :, :total], ns[slot, :, total:] = split(out)

    def remains(i):
        slot = i % 2
        h, l = ns[slot, :, :total], ns[slot, :, total:]
        rem = dot(h, lh[...]) + dot(l, lh[...]) + dot(h, ll[...])
        sq = rem * rem
        for k in range(tile // LEAF):
            leaf = i * (tile // LEAF) + k
            sums[leaf : leaf + 1, :] = jnp.sum(
                sq[k * LEAF : (k + 1) * LEAF, :], axis=0, keepdims=True
            )

    stores = [
        pltpu.make_async_copy(n_v.at[at(i)], n_hbm.at[at(i)], n_sem.at[i]) for i in range(chunks)
    ]
    prepare(0)
    for i in range(chunks):
        product(i)
        if i + 1 < chunks:
            prepare(i + 1)
        if i:
            stores[i - 1].start()
            remains(i - 1)
    stores[-1].start()
    remains(chunks - 1)
    pick = (
        lax.broadcasted_iota(jnp.int32, (rounds, total), 1) // columns
        == lax.broadcasted_iota(jnp.int32, (rounds, total), 0)
    ).astype(F32)
    q_ref[...] = jnp.sqrt(total_leaves * exact(pick, sums[...], NT) / energy)
    for c in stores:
        c.wait()


def local(prior_basis, samples):
    rounds, rows, columns = samples.shape
    basis = prior_basis.shape[1]
    total = rounds * columns
    leaves = rows // LEAF
    total_leaves = leaves * lax.axis_size("row")
    samples = jnp.swapaxes(samples, 1, 2)
    stat = all_sum(prior_basis, samples)
    depth = basis + total
    chunk = min(TILE, rows)
    vmem = pl.BlockSpec(memory_space=pltpu.VMEM)
    hbm = pl.BlockSpec(memory_space=pl.ANY)
    sem = pltpu.SemaphoreType.DMA((rows // chunk,))
    return pl.pallas_call(
        functools.partial(finish_kernel, columns, total_leaves),
        in_specs=[vmem, hbm, hbm],
        out_specs=(hbm, vmem),
        out_shape=(
            jax.ShapeDtypeStruct((rows, total), F32),
            jax.ShapeDtypeStruct((rounds, leaves), F32),
        ),
        scratch_shapes=[
            pltpu.VMEM((rows, basis), F32),
            pltpu.VMEM((rounds, columns, rows), F32),
            pltpu.VMEM((rows, total), F32),
            pltpu.VMEM((total, 2 * total), F32),
            pltpu.VMEM((total, total), F32),
            pltpu.VMEM((2, chunk, 2 * depth), BF16),
            pltpu.VMEM((2, chunk, 2 * total), BF16),
            pltpu.VMEM((depth, total), BF16),
            pltpu.VMEM((depth, total), BF16),
            pltpu.VMEM((total, total), BF16),
            pltpu.VMEM((total, total), BF16),
            pltpu.VMEM((leaves, total), F32),
            sem,
            sem,
            sem,
        ],
        name="finish",
    )(stat, prior_basis, samples)


def solution(mesh):
    in_specs = (P(("grp", "row"), None), P(None, ("grp", "row"), None))
    out_specs = (P(("grp", "row"), None), P(None, ("grp", "row")))
    return jax.shard_map(local, mesh=mesh, in_specs=in_specs, out_specs=out_specs, check_vma=False)
```
